8 devices in a mesh: data: 2 (over z, y), time: 4 (over x, core).
Axes of the slice: x: 2, y: 2, z: 1, core: 2. Of those that a mesh axis runs over, the one named last changes fastest.
Arguments:
- x_init: float32 [128, 256, 16], P('data'), parts along dimension 0
- w_in: bfloat16 [16, 1152], replicated
- w_out: bfloat16 [1152, 16], replicated
- mod_scale: bfloat16 [4, 1152], P('time')
- mod_shift: bfloat16 [4, 1152], P('time')
- step_size: float32 [4], P('time')
Outputs:
- output: float32 [4, 128, 256, 16], P('time', 'data'), parts along dimension 1
There are 2 independent parts. The reference program is written for one: setup_inputs(seed, part) draws one part's arguments, and reference() takes and returns one part's arrays. A program takes and returns all parts, laid end to end along the dimension named above; an argument that names none is the same for every part.
All inputs are finite; a program needn't handle non-finite values.
Results may differ from the reference program's by a relative error of at most 0.001.
Values are sent between devices in bfloat16 or wider.
A program may use at most 1 GiB of HBM per device.

```python
import jax
import jax.numpy as jnp
from jax import lax

BATCH = 64
TOKENS = 256
CHANNELS = 16
HIDDEN = 1152
STEPS = 4
SWEEPS = 4


def setup_inputs(seed: int = 0, part: int = 0) -> dict:
    key_list = jax.random.split(jax.random.key(seed), 7)
    x_init = jax.random.normal(jax.random.fold_in(key_list[0], part), (BATCH, TOKENS, CHANNELS), jnp.float32)
    w_in = jax.random.normal(key_list[1], (CHANNELS, HIDDEN), jnp.float32) * (CHANNELS * STEPS) ** -0.5
    w_raw = jax.random.normal(key_list[2], (HIDDEN, CHANNELS), jnp.float32)
    w_out = (w_raw - jnp.mean(w_raw, axis=0, keepdims=True)) * (1.5 * HIDDEN ** -0.5)
    time_pos = (jnp.arange(STEPS, dtype=jnp.float32) + 0.5) / STEPS
    mode_coef = 0.4 * jax.random.normal(key_list[3], (3, HIDDEN), jnp.float32)
    mod_scale = (mode_coef[0][None, :] + mode_coef[1][None, :] * jnp.cos(jnp.pi * time_pos)[:, None] + mode_coef[2][None, :] * jnp.cos(2.0 * jnp.pi * time_pos)[:, None] + 0.1 * jax.random.normal(key_list[4], (STEPS, HIDDEN), jnp.float32))
    mod_shift = jax.random.normal(key_list[5], (STEPS, HIDDEN), jnp.float32)
    step_size = jax.random.uniform(key_list[6], (STEPS,), jnp.float32, 0.5, 1.5) * STEPS ** -0.5
    return {"x_init": x_init, "w_in": w_in.astype(jnp.bfloat16), "w_out": w_out.astype(jnp.bfloat16), "mod_scale": mod_scale.astype(jnp.bfloat16), "mod_shift": mod_shift.astype(jnp.bfloat16), "step_size": step_size}


def denoise(latent, w_in, w_out, scale_row, shift_row):
    flat_in = latent.astype(jnp.bfloat16).reshape(-1, latent.shape[-1])
    pre_act = jnp.dot(flat_in, w_in, preferred_element_type=jnp.float32)
    hidden_act = jax.nn.gelu(pre_act * (1.0 + scale_row.astype(jnp.float32)) + shift_row.astype(jnp.float32), approximate=True)
    return jnp.dot(hidden_act.astype(jnp.bfloat16), w_out, preferred_element_type=jnp.float32).reshape(latent.shape)


def reference(x_init, w_in, w_out, mod_scale, mod_shift, step_size):
    def one_step_drift(item):
        return denoise(item[0], w_in, w_out, item[1], item[2])

    def one_sweep(latents, unused):
        drifts = lax.map(one_step_drift, (latents, mod_scale, mod_shift))
        increments = step_size[:-1, None, None, None] * (0.5 * (drifts[:-1] + drifts[1:]))
        running = jnp.cumsum(increments, axis=0)
        return jnp.concatenate([x_init[None], x_init[None] + running], axis=0), unused

    start = jnp.broadcast_to(x_init[None], (STEPS,) + x_init.shape)
    final, unused_out = lax.scan(one_sweep, start, None, length=SWEEPS)
    return final
```

```python
import functools

import jax
import jax.numpy as jnp
from jax import lax
from jax.experimental import pallas as pl
from jax.experimental.pallas import tpu as pltpu
from jax.sharding import PartitionSpec as P

SWEEPS = 4
N_TIME = 4
CH = 16
TOK = 256
HIDDEN = 1152
BLOCK = 384
LAG = 2
GROUP = 2
GROUP_A = 4
DEPTH = 10 * CH
SQRT_2_PI = 0.7978845608028654
LINEAR = 2.0 * SQRT_2_PI
CUBIC = 8.0 * 0.044715 * SQRT_2_PI
MESH = pl.DeviceIdType.MESH
UP = 2.0**64
DOWN = 2.0**-64
SPLIT = 2.0**32


def modulated_weights(w_in, scale, shift):
    half = 0.5 * (1.0 + scale.astype(jnp.float32))
    w = w_in.astype(jnp.float32)
    w_down = w * DOWN
    low = w * half
    middle = w_down * half
    high = w_down * (half * DOWN)
    in_high = jnp.abs(high) >= SPLIT
    in_middle = jnp.logical_and(jnp.abs(middle) >= SPLIT, jnp.logical_not(in_high))
    in_low = jnp.logical_not(jnp.logical_or(in_middle, in_high))
    rows = []
    for chosen, value in ((in_low, low), (in_middle, middle), (in_high, high)):
        rest = jnp.where(chosen, value, 0.0)
        for _ in range(3):
            part = rest.astype(jnp.bfloat16)
            rest = rest - part.astype(jnp.float32)
            rows.append(part)
    first_row = lax.broadcasted_iota(jnp.int32, (CH, HIDDEN), 0) == 0
    half_shift = jnp.broadcast_to(0.5 * shift.astype(jnp.float32), (CH, HIDDEN))
    rows.append(jnp.where(first_row, half_shift, 0.0).astype(jnp.bfloat16))
    return jnp.concatenate(rows, axis=0).T


def first_rhs(latent, ones):
    top = float(jnp.finfo(jnp.bfloat16).max)
    x = latent.astype(jnp.bfloat16)
    up = jnp.clip(x * UP, -top, top)
    up_up = jnp.clip(up * UP, -top, top)
    return jnp.concatenate([x, x, x, up, up, up, up_up, up_up, up_up, ones], axis=0)


def activation(half_pre):
    cubic = half_pre * (half_pre * half_pre * CUBIC + LINEAR)
    return (half_pre * jnp.tanh(cubic) + half_pre).astype(jnp.bfloat16)


def run_evals(evals, lhs, w_out_ref, done):
    n_blocks = HIDDEN // BLOCK
    steps = [(e, b) for e in range(len(evals)) for b in range(n_blocks)]
    pre, rhs, acc = {}, {}, {}

    def issue(i):
        e, b = steps[i]
        if b == 0:
            rhs[e] = evals[e][2]()
        pre[i] = jnp.dot(lhs(evals[e][1], b), rhs[e], preferred_element_type=jnp.float32)

    for i in range(min(LAG, len(steps))):
        issue(i)
    for i, (e, b) in enumerate(steps):
        if i + LAG < len(steps):
            issue(i + LAG)
        hidden = activation(pre.pop(i))
        part = jnp.dot(w_out_ref[:, b * BLOCK:(b + 1) * BLOCK], hidden, preferred_element_type=jnp.float32)
        acc[e] = part if b == 0 else acc[e] + part
        if b == n_blocks - 1:
            done(evals[e][0], acc.pop(e))


def kernel(n_lat, x_hbm, w_in_ref, w_out_ref, scale_ref, shift_ref, step_ref, out_hbm,
           x_own, x_all, lhs_ref, drift0, stage, scales, shifts, steps_buf,
           load_sem, pass_sem, own_sem, par_send, par_recv, send_sem, recv_sem):
    me = lax.axis_index("time")
    others = [lax.rem(me + k, N_TIME) for k in range(1, N_TIME)]
    n_own = n_lat // N_TIME
    n_groups = n_own // GROUP

    load = pltpu.make_async_copy(x_hbm.at[pl.ds(me * n_own, n_own)], x_own, load_sem)
    load.start()
    steps_buf[me] = jnp.full((8, 128), 0.5 * step_ref[0], jnp.float32)
    barrier = pltpu.get_barrier_semaphore()
    for peer in others:
        pl.semaphore_signal(barrier, inc=1, device_id={"time": peer}, device_id_type=MESH)

    @pl.when(me == 0)
    def _():
        pltpu.make_async_copy(x_hbm, x_all, pass_sem).start()

    scales[me] = scale_ref[...]
    shifts[me] = shift_ref[...]
    lhs_ref[me] = modulated_weights(w_in_ref[...], scale_ref[...], shift_ref[...])
    pl.semaphore_wait(barrier, N_TIME - 1)

    def param_copies(slot, peer):
        return [
            pltpu.make_async_remote_copy(
                src_ref=src, dst_ref=dst.at[slot], send_sem=par_send.at[i, peer], recv_sem=par_recv.at[i, slot],
                device_id={"time": peer}, device_id_type=MESH)
            for i, (src, dst) in enumerate(((scale_ref, scales), (shift_ref, shifts), (steps_buf.at[slot], steps_buf)))
        ]

    for peer in others:
        for copy in param_copies(me, peer):
            copy.start()
    load.wait()

    ones = (lax.broadcasted_iota(jnp.int32, (CH, TOK), 0) == 0).astype(jnp.float32).astype(jnp.bfloat16)

    def lhs(timestep, block):
        return lhs_ref[timestep, block * BLOCK:(block + 1) * BLOCK, :]

    def own_pass(trip, carry):
        base = trip * GROUP_A
        evals = [(base + g, me, functools.partial(lambda i: first_rhs(x_own[i], ones), base + g)) for g in range(GROUP_A)]

        def done(i, drift):
            drift0[me, i] = drift

        run_evals(evals, lhs, w_out_ref, done)
        return carry

    lax.fori_loop(0, n_own // GROUP_A, own_pass, 0)

    @pl.when(me == 0)
    def _():
        pltpu.make_async_copy(x_hbm, x_all, pass_sem).wait()
        pltpu.make_async_copy(x_all, out_hbm, pass_sem).start()

    for peer in others:
        for copy in param_copies(peer, peer):
            copy.wait_recv()
    for peer in others:
        lhs_ref[peer] = modulated_weights(w_in_ref[...], scales[peer], shifts[peer])
    half_step = [steps_buf[j, 0:1, 0:1] for j in range(N_TIME - 1)]

    def data_copy(group, slot, peer):
        rows = pl.ds(group * GROUP, GROUP)
        return pltpu.make_async_remote_copy(
            src_ref=stage.at[peer, rows], dst_ref=out_hbm.at[pl.ds(slot * n_own + group * GROUP, GROUP)],
            send_sem=send_sem.at[group, peer], recv_sem=recv_sem.at[group, slot],
            device_id={"time": peer}, device_id_type=MESH)

    def own_copy(group):
        return pltpu.make_async_copy(stage.at[me, pl.ds(group * GROUP, GROUP)],
                                     out_hbm.at[pl.ds(me * n_own + group * GROUP, GROUP)], own_sem.at[group])

    def sweeps(group, carry):
        base = group * GROUP
        x0 = [x_own[base + g] for g in range(GROUP)]
        drifts = {}
        evals = []
        rhs0 = {}

        def start_rhs(g):
            if g not in rhs0:
                rhs0[g] = first_rhs(x0[g], ones)
            return rhs0[g]

        def latent(sweep, j, g):
            total = x0[g]
            for i in range(j):
                total = total + half_step[i] * (drifts[sweep, i, g] + drifts[sweep, i + 1, g])
            return total

        for k in range(N_TIME - 1):
            for g in range(GROUP):
                evals.append((("first", k, g), others[k], functools.partial(start_rhs, g)))
        for sweep in range(1, SWEEPS):
            for g in range(GROUP):
                for j in range(1, N_TIME):
                    evals.append(((sweep, j, g), j, functools.partial(
                        lambda s, j, g: first_rhs(latent(s - 1, j, g), ones), sweep, j, g)))

        def done(key, drift):
            if key[0] == "first":
                _, k, g = key
                drift0[others[k], base + g] = drift
                if k == N_TIME - 2:
                    for j in range(N_TIME):
                        drifts[0, j, g] = drift0[j, base + g]
                        if j == 0:
                            for sweep in range(1, SWEEPS):
                                drifts[sweep, 0, g] = drifts[0, 0, g]
            else:
                sweep, j, g = key
                drifts[sweep, j, g] = drift
                if sweep == SWEEPS - 1:
                    stage[j, base + g] = latent(sweep, j, g)

        run_evals(evals, lhs, w_out_ref, done)
        for peer in others:
            @pl.when(peer != 0)
            def _(peer=peer):
                data_copy(group, me, peer).start()

        @pl.when(me != 0)
        def _():
            own_copy(group).start()

        return carry

    lax.fori_loop(0, n_groups, sweeps, 0)

    for peer in others:
        for copy in param_copies(me, peer):
            copy.wait_send()

    @pl.when(me == 0)
    def _():
        pltpu.make_async_copy(x_all, out_hbm, pass_sem).wait()

    def finish(group, carry):
        for peer in others:
            @pl.when(peer != 0)
            def _(peer=peer):
                data_copy(group, me, peer).wait_send()

        @pl.when(me != 0)
        def _():
            own_copy(group).wait()
            for peer in others:
                data_copy(group, peer, peer).wait_recv()

        return carry

    lax.fori_loop(0, n_groups, finish, 0)


def solution(mesh):
    def local(x_init, w_in, w_out, mod_scale, mod_shift, step_size):
        n_lat = x_init.shape[0]
        n_own = n_lat // N_TIME
        n_groups = n_own // GROUP
        vmem = pl.BlockSpec(memory_space=pltpu.VMEM)
        out = pl.pallas_call(
            functools.partial(kernel, n_lat),
            out_shape=jax.ShapeDtypeStruct((n_lat, CH, TOK), jnp.float32),
            in_specs=[pl.BlockSpec(memory_space=pl.ANY), vmem, vmem, vmem, vmem, pl.BlockSpec(memory_space=pltpu.SMEM)],
            out_specs=pl.BlockSpec(memory_space=pl.ANY),
            scratch_shapes=[
                pltpu.VMEM((n_own, CH, TOK), jnp.float32),
                pltpu.VMEM((n_lat, CH, TOK), jnp.float32),
                pltpu.VMEM((N_TIME, HIDDEN, DEPTH), jnp.bfloat16),
                pltpu.VMEM((N_TIME, n_own, CH, TOK), jnp.float32),
                pltpu.VMEM((N_TIME, n_own, CH, TOK), jnp.float32),
                pltpu.VMEM((N_TIME, 1, HIDDEN), jnp.bfloat16),
                pltpu.VMEM((N_TIME, 1, HIDDEN), jnp.bfloat16),
                pltpu.VMEM((N_TIME, 8, 128), jnp.float32),
                pltpu.SemaphoreType.DMA,
                pltpu.SemaphoreType.DMA,
                pltpu.SemaphoreType.DMA((n_groups,)),
                pltpu.SemaphoreType.DMA((3, N_TIME)),
                pltpu.SemaphoreType.DMA((3, N_TIME)),
                pltpu.SemaphoreType.DMA((n_groups, N_TIME)),
                pltpu.SemaphoreType.DMA((n_groups, N_TIME)),
            ],
            compiler_params=pltpu.CompilerParams(collective_id=0, has_side_effects=True, vmem_limit_bytes=48 * 1024 * 1024),
        )(jnp.transpose(x_init, (0, 2, 1)), w_in, w_out.T, mod_scale, mod_shift, step_size)
        return jnp.transpose(out, (0, 2, 1))[None]

    return jax.shard_map(local, mesh=mesh, in_specs=(P("data"), P(), P(), P("time"), P("time"), P("time")), out_specs=P("time", "data"), check_vma=False)
```

```python
import functools

import jax
import jax.numpy as jnp
from jax import lax
from jax.experimental import pallas as pl
from jax.experimental.pallas import tpu as pltpu
from jax.sharding import PartitionSpec as P

SWEEPS = 4
N_TIME = 4
CH = 16
TOK = 256
HIDDEN = 1152
BLOCK = 384
LAG = 2
GROUP = 2
GROUP_A = 4
DEPTH = 10 * CH
SQRT_2_PI = 0.7978845608028654
LINEAR = 2.0 * SQRT_2_PI
CUBIC = 8.0 * 0.044715 * SQRT_2_PI
MESH = pl.DeviceIdType.MESH
UP = 2.0**64
DOWN = 2.0**-64
SPLIT = 2.0**32


def modulated_weights(w_in, scale, shift):
    half = 0.5 * (1.0 + scale.astype(jnp.float32))
    w = w_in.astype(jnp.float32)
    w_down = w * DOWN
    low = w * half
    middle = w_down * half
    high = w_down * (half * DOWN)
    in_high = jnp.abs(high) >= SPLIT
    in_middle = jnp.logical_and(jnp.abs(middle) >= SPLIT, jnp.logical_not(in_high))
    in_low = jnp.logical_not(jnp.logical_or(in_middle, in_high))
    rows = []
    for chosen, value in ((in_low, low), (in_middle, middle), (in_high, high)):
        rest = jnp.where(chosen, value, 0.0)
        for _ in range(3):
            part = rest.astype(jnp.bfloat16)
            rest = rest - part.astype(jnp.float32)
            rows.append(part)
    first_row = lax.broadcasted_iota(jnp.int32, (CH, HIDDEN), 0) == 0
    half_shift = jnp.broadcast_to(0.5 * shift.astype(jnp.float32), (CH, HIDDEN))
    rows.append(jnp.where(first_row, half_shift, 0.0).astype(jnp.bfloat16))
    return jnp.concatenate(rows, axis=0).T


def first_rhs(latent, ones):
    top = float(jnp.finfo(jnp.bfloat16).max)
    x = latent.astype(jnp.bfloat16)
    up = jnp.clip(x * UP, -top, top)
    up_up = jnp.clip(up * UP, -top, top)
    return jnp.concatenate([x, x, x, up, up, up, up_up, up_up, up_up, ones], axis=0)


def activation(half_pre):
    cubic = half_pre * (half_pre * half_pre * CUBIC + LINEAR)
    return (half_pre * jnp.tanh(cubic) + half_pre).astype(jnp.bfloat16)


def run_evals(evals, lhs, w_out_ref, done):
    n_blocks = HIDDEN // BLOCK
    steps = [(e, b) for e in range(len(evals)) for b in range(n_blocks)]
    pre, rhs, acc = {}, {}, {}

    def issue(i):
        e, b = steps[i]
        if b == 0:
            rhs[e] = evals[e][2]()
        pre[i] = jnp.dot(lhs(evals[e][1], b), rhs[e], preferred_element_type=jnp.float32)

    for i in range(min(LAG, len(steps))):
        issue(i)
    for i, (e, b) in enumerate(steps):
        if i + LAG < len(steps):
            issue(i + LAG)
        hidden = activation(pre.pop(i))
        part = jnp.dot(w_out_ref[:, b * BLOCK:(b + 1) * BLOCK], hidden, preferred_element_type=jnp.float32)
        acc[e] = part if b == 0 else acc[e] + part
        if b == n_blocks - 1:
            done(evals[e][0], acc.pop(e))


def kernel(n_lat, x_hbm, w_in_hbm, w_out_hbm, scale_hbm, shift_hbm, step_hbm, out_hbm,
           w_in_ref, w_out_ref, x_own, x_all, lhs_ref, drift0, stage, scales, shifts, steps_buf,
           load_sem, pass_sem, own_sem, par_send, par_recv, send_sem, recv_sem):
    me = lax.axis_index("time")
    others = [lax.rem(me + k, N_TIME) for k in range(1, N_TIME)]
    n_own = n_lat // N_TIME
    n_groups = n_own // GROUP

    loads = [
        pltpu.make_async_copy(src, dst, load_sem.at[i])
        for i, (src, dst) in enumerate((
            (scale_hbm, scales.at[me]), (shift_hbm, shifts.at[me]), (step_hbm, steps_buf.at[me]),
            (w_in_hbm, w_in_ref), (x_hbm.at[pl.ds(me * n_own, n_own)], x_own), (w_out_hbm, w_out_ref)))
    ]
    for load in loads:
        load.start()
    barrier = pltpu.get_barrier_semaphore()
    for peer in others:
        pl.semaphore_signal(barrier, inc=1, device_id={"time": peer}, device_id_type=MESH)

    @pl.when(me == 0)
    def _():
        pltpu.make_async_copy(x_hbm, x_all, pass_sem).start()

    for load in loads:
        load.wait()
    pl.semaphore_wait(barrier, N_TIME - 1)

    def param_copies(slot, peer):
        return [
            pltpu.make_async_remote_copy(
                src_ref=dst.at[slot], dst_ref=dst.at[slot], send_sem=par_send.at[i, peer], recv_sem=par_recv.at[i, slot],
                device_id={"time": peer}, device_id_type=MESH)
            for i, dst in enumerate((scales, shifts, steps_buf))
        ]

    for peer in others:
        for copy in param_copies(me, peer):
            copy.start()
    lhs_ref[me] = modulated_weights(w_in_ref[...], scales[me], shifts[me])

    ones = (lax.broadcasted_iota(jnp.int32, (CH, TOK), 0) == 0).astype(jnp.float32).astype(jnp.bfloat16)

    def lhs(timestep, block):
        return lhs_ref[timestep, block * BLOCK:(block + 1) * BLOCK, :]

    def own_pass(trip, carry):
        base = trip * GROUP_A
        evals = [(base + g, me, functools.partial(lambda i: first_rhs(x_own[i], ones), base + g)) for g in range(GROUP_A)]

        def done(i, drift):
            drift0[me, i] = drift

        run_evals(evals, lhs, w_out_ref, done)
        return carry

    lax.fori_loop(0, n_own // GROUP_A, own_pass, 0)

    @pl.when(me == 0)
    def _():
        pltpu.make_async_copy(x_hbm, x_all, pass_sem).wait()
        pltpu.make_async_copy(x_all, out_hbm, pass_sem).start()

    for peer in others:
        for copy in param_copies(peer, peer):
            copy.wait_recv()
    for peer in others:
        lhs_ref[peer] = modulated_weights(w_in_ref[...], scales[peer], shifts[peer])
    half_step = [0.5 * steps_buf[j] for j in range(N_TIME - 1)]

    def data_copy(group, slot, peer):
        rows = pl.ds(group * GROUP, GROUP)
        return pltpu.make_async_remote_copy(
            src_ref=stage.at[peer, rows], dst_ref=out_hbm.at[pl.ds(slot * n_own + group * GROUP, GROUP)],
            send_sem=send_sem.at[group, peer], recv_sem=recv_sem.at[group, slot],
            device_id={"time": peer}, device_id_type=MESH)

    def own_copy(group):
        return pltpu.make_async_copy(stage.at[me, pl.ds(group * GROUP, GROUP)],
                                     out_hbm.at[pl.ds(me * n_own + group * GROUP, GROUP)], own_sem.at[group])

    def sweeps(group, carry):
        base = group * GROUP
        x0 = [x_own[base + g] for g in range(GROUP)]
        drifts = {}
        evals = []
        rhs0 = {}

        def start_rhs(g):
            if g not in rhs0:
                rhs0[g] = first_rhs(x0[g], ones)
            return rhs0[g]

        def latent(sweep, j, g):
            total = x0[g]
            for i in range(j):
                total = total + half_step[i] * (drifts[sweep, i, g] + drifts[sweep, i + 1, g])
            return total

        for k in range(N_TIME - 1):
            for g in range(GROUP):
                evals.append((("first", k, g), others[k], functools.partial(start_rhs, g)))
        for sweep in range(1, SWEEPS):
            for g in range(GROUP):
                for j in range(1, N_TIME):
                    evals.append(((sweep, j, g), j, functools.partial(
                        lambda s, j, g: first_rhs(latent(s - 1, j, g), ones), sweep, j, g)))

        def done(key, drift):
            if key[0] == "first":
                _, k, g = key
                drift0[others[k], base + g] = drift
                if k == N_TIME - 2:
                    for j in range(N_TIME):
                        drifts[0, j, g] = drift0[j, base + g]
                        if j == 0:
                            for sweep in range(1, SWEEPS):
                                drifts[sweep, 0, g] = drifts[0, 0, g]
            else:
                sweep, j, g = key
                drifts[sweep, j, g] = drift
                if sweep == SWEEPS - 1:
                    stage[j, base + g] = latent(sweep, j, g)

        run_evals(evals, lhs, w_out_ref, done)
        for peer in others:
            @pl.when(peer != 0)
            def _(peer=peer):
                data_copy(group, me, peer).start()

        @pl.when(me != 0)
        def _():
            own_copy(group).start()

        return carry

    lax.fori_loop(0, n_groups, sweeps, 0)

    for peer in others:
        for copy in param_copies(me, peer):
            copy.wait_send()

    @pl.when(me == 0)
    def _():
        pltpu.make_async_copy(x_all, out_hbm, pass_sem).wait()

    def finish(group, carry):
        for peer in others:
            @pl.when(peer != 0)
            def _(peer=peer):
                data_copy(group, me, peer).wait_send()

        @pl.when(me != 0)
        def _():
            own_copy(group).wait()
            for peer in others:
                data_copy(group, peer, peer).wait_recv()

        return carry

    lax.fori_loop(0, n_groups, finish, 0)


def solution(mesh):
    def local(x_init, w_in, w_out, mod_scale, mod_shift, step_size):
        n_lat = x_init.shape[0]
        n_own = n_lat // N_TIME
        n_groups = n_own // GROUP
        out = pl.pallas_call(
            functools.partial(kernel, n_lat),
            out_shape=jax.ShapeDtypeStruct((n_lat, CH, TOK), jnp.float32),
            in_specs=[pl.BlockSpec(memory_space=pltpu.HBM)] * 6,
            out_specs=pl.BlockSpec(memory_space=pl.ANY),
            scratch_shapes=[
                pltpu.VMEM((CH, HIDDEN), jnp.bfloat16),
                pltpu.VMEM((CH, HIDDEN), jnp.bfloat16),
                pltpu.VMEM((n_own, CH, TOK), jnp.float32),
                pltpu.VMEM((n_lat, CH, TOK), jnp.float32),
                pltpu.VMEM((N_TIME, HIDDEN, DEPTH), jnp.bfloat16),
                pltpu.VMEM((N_TIME, n_own, CH, TOK), jnp.float32),
                pltpu.VMEM((N_TIME, n_own, CH, TOK), jnp.float32),
                pltpu.VMEM((N_TIME, 1, HIDDEN), jnp.bfloat16),
                pltpu.VMEM((N_TIME, 1, HIDDEN), jnp.bfloat16),
                pltpu.VMEM((N_TIME, 1, 1), jnp.float32),
                pltpu.SemaphoreType.DMA((6,)),
                pltpu.SemaphoreType.DMA,
                pltpu.SemaphoreType.DMA((n_groups,)),
                pltpu.SemaphoreType.DMA((3, N_TIME)),
                pltpu.SemaphoreType.DMA((3, N_TIME)),
                pltpu.SemaphoreType.DMA((n_groups, N_TIME)),
                pltpu.SemaphoreType.DMA((n_groups, N_TIME)),
            ],
            compiler_params=pltpu.CompilerParams(collective_id=0, has_side_effects=True, vmem_limit_bytes=67_043_328),
        )(jnp.transpose(x_init, (0, 2, 1)), w_in, w_out.T, mod_scale, mod_shift, step_size[:, None])
        return jnp.transpose(out, (0, 2, 1))[None]

    return jax.shard_map(local, mesh=mesh, in_specs=(P("data"), P(), P(), P("time"), P("time"), P("time")), out_specs=P("time", "data"), check_vma=False)
```

```python
import functools

import jax
import jax.numpy as jnp
from jax import lax
from jax.experimental import pallas as pl
from jax.experimental.pallas import tpu as pltpu
from jax.sharding import PartitionSpec as P

SWEEPS = 4
N_TIME = 4
CH = 16
TOK = 256
HIDDEN = 1152
BLOCK = 128
LAG = 5
GROUP = 2
GROUP_A = 8
DEPTH = 8 * CH
SQRT_2_PI = 0.7978845608028654
LINEAR = 2.0 * SQRT_2_PI
CUBIC = 8.0 * 0.044715 * SQRT_2_PI
MESH = pl.DeviceIdType.MESH
UP = 2.0**64
DOWN = 2.0**-64
SPLIT = 0.5


def modulated_weights(w_in, scale, shift):
    half = 0.5 * (1.0 + scale.astype(jnp.float32))
    w = w_in.astype(jnp.float32)
    low = w * half
    high = (w * DOWN) * (half * DOWN)
    in_high = jnp.abs(high) >= SPLIT
    rows = []
    for chosen, value in ((jnp.logical_not(in_high), low), (in_high, high)):
        rest = jnp.where(chosen, value, 0.0)
        for _ in range(3):
            part = rest.astype(jnp.bfloat16)
            rest = rest - part.astype(jnp.float32)
            rows.append(part)
    first_row = lax.broadcasted_iota(jnp.int32, (CH, HIDDEN), 0) == 0
    half_shift = jnp.broadcast_to(0.5 * shift.astype(jnp.float32), (CH, HIDDEN))
    rows.append(jnp.where(first_row, half_shift, 0.0).astype(jnp.bfloat16))
    rows.append(jnp.zeros((CH, HIDDEN), jnp.bfloat16))
    return jnp.concatenate(rows, axis=0).T


def first_rhs(latent, ones):
    top = float(jnp.finfo(jnp.bfloat16).max)
    x = latent.astype(jnp.bfloat16)
    up = jnp.clip(x * UP * UP, -top, top)
    return jnp.concatenate([x, x, x, up, up, up, ones, jnp.zeros_like(ones)], axis=0)


def activation(half_pre):
    cubic = half_pre * (half_pre * half_pre * CUBIC + LINEAR)
    return (half_pre * jnp.tanh(cubic) + half_pre).astype(jnp.bfloat16)


def run_evals(evals, lhs, w_out_ref, done):
    n_blocks = HIDDEN // BLOCK
    steps = [(e, b) for e in range(len(evals)) for b in range(n_blocks)]
    pre, rhs, acc = {}, {}, {}

    def issue(i):
        e, b = steps[i]
        if b == 0:
            rhs[e] = evals[e][2]()
        pre[i] = jnp.dot(lhs(evals[e][1], b), rhs[e], preferred_element_type=jnp.float32)

    for i in range(min(LAG, len(steps))):
        issue(i)
    for i, (e, b) in enumerate(steps):
        if i + LAG < len(steps):
            issue(i + LAG)
        hidden = activation(pre.pop(i))
        part = jnp.dot(w_out_ref[:, b * BLOCK:(b + 1) * BLOCK], hidden, preferred_element_type=jnp.float32)
        acc[e] = part if b == 0 else acc[e] + part
        if b == n_blocks - 1:
            done(evals[e][0], acc.pop(e))


def kernel(n_lat, x_hbm, w_in_hbm, w_out_hbm, scale_hbm, shift_hbm, step_hbm, out_hbm,
           w_in_ref, w_out_ref, x_own, x_all, lhs_ref, drift0, stage, scales, shifts, steps_buf,
           load_sem, pass_sem, own_sem, par_send, par_recv, send_sem, recv_sem):
    me = lax.axis_index("time")
    others = [lax.rem(me + k, N_TIME) for k in range(1, N_TIME)]
    n_own = n_lat // N_TIME
    n_groups = n_own // GROUP

    loads = [
        pltpu.make_async_copy(src, dst, load_sem.at[i])
        for i, (src, dst) in enumerate((
            (scale_hbm, scales.at[me]), (shift_hbm, shifts.at[me]), (step_hbm, steps_buf.at[me]),
            (w_in_hbm, w_in_ref), (x_hbm.at[pl.ds(me * n_own, n_own)], x_own), (w_out_hbm, w_out_ref)))
    ]
    for load in loads:
        load.start()
    barrier = pltpu.get_barrier_semaphore()
    for peer in others:
        pl.semaphore_signal(barrier, inc=1, device_id={"time": peer}, device_id_type=MESH)

    @pl.when(me == 0)
    def _():
        pltpu.make_async_copy(x_hbm, x_all, pass_sem).start()

    for load in loads:
        load.wait()
    pl.semaphore_wait(barrier, N_TIME - 1)

    def param_copies(slot, peer):
        return [
            pltpu.make_async_remote_copy(
                src_ref=dst.at[slot], dst_ref=dst.at[slot], send_sem=par_send.at[i, peer], recv_sem=par_recv.at[i, slot],
                device_id={"time": peer}, device_id_type=MESH)
            for i, dst in enumerate((scales, shifts, steps_buf))
        ]

    for peer in others:
        for copy in param_copies(me, peer):
            copy.start()
    lhs_ref[me] = modulated_weights(w_in_ref[...], scales[me], shifts[me])

    ones = (lax.broadcasted_iota(jnp.int32, (CH, TOK), 0) == 0).astype(jnp.float32).astype(jnp.bfloat16)

    def lhs(timestep, block):
        return lhs_ref[timestep, block * BLOCK:(block + 1) * BLOCK, :]

    def own_pass(trip, carry):
        base = trip * GROUP_A
        evals = [(base + g, me, functools.partial(lambda i: first_rhs(x_own[i], ones), base + g)) for g in range(GROUP_A)]

        def done(i, drift):
            drift0[me, i] = drift

        run_evals(evals, lhs, w_out_ref, done)
        return carry

    lax.fori_loop(0, n_own // GROUP_A, own_pass, 0)

    @pl.when(me == 0)
    def _():
        pltpu.make_async_copy(x_hbm, x_all, pass_sem).wait()
        pltpu.make_async_copy(x_all, out_hbm, pass_sem).start()

    for peer in others:
        for copy in param_copies(peer, peer):
            copy.wait_recv()
    for peer in others:
        lhs_ref[peer] = modulated_weights(w_in_ref[...], scales[peer], shifts[peer])
    half_step = [0.5 * steps_buf[j] for j in range(N_TIME - 1)]

    def data_copy(group, slot, peer):
        rows = pl.ds(group * GROUP, GROUP)
        return pltpu.make_async_remote_copy(
            src_ref=stage.at[peer, rows], dst_ref=out_hbm.at[pl.ds(slot * n_own + group * GROUP, GROUP)],
            send_sem=send_sem.at[group, peer], recv_sem=recv_sem.at[group, slot],
            device_id={"time": peer}, device_id_type=MESH)

    def own_copy(group):
        return pltpu.make_async_copy(stage.at[me, pl.ds(group * GROUP, GROUP)],
                                     out_hbm.at[pl.ds(me * n_own + group * GROUP, GROUP)], own_sem.at[group])

    def sweeps(group, carry):
        base = group * GROUP
        x0 = [x_own[base + g] for g in range(GROUP)]
        drifts = {}
        evals = []
        rhs0 = {}

        def start_rhs(g):
            if g not in rhs0:
                rhs0[g] = first_rhs(x0[g], ones)
            return rhs0[g]

        def latent(sweep, j, g):
            total = x0[g]
            for i in range(j):
                total = total + half_step[i] * (drifts[sweep, i, g] + drifts[sweep, i + 1, g])
            return total

        for k in range(N_TIME - 1):
            for g in range(GROUP):
                evals.append((("first", k, g), others[k], functools.partial(start_rhs, g)))
        for sweep in range(1, SWEEPS):
            for g in range(GROUP):
                for j in range(1, N_TIME):
                    evals.append(((sweep, j, g), j, functools.partial(
                        lambda s, j, g: first_rhs(latent(s - 1, j, g), ones), sweep, j, g)))

        def done(key, drift):
            if key[0] == "first":
                _, k, g = key
                drift0[others[k], base + g] = drift
                if k == N_TIME - 2:
                    for j in range(N_TIME):
                        drifts[0, j, g] = drift0[j, base + g]
                        if j == 0:
                            for sweep in range(1, SWEEPS):
                                drifts[sweep, 0, g] = drifts[0, 0, g]
            else:
                sweep, j, g = key
                drifts[sweep, j, g] = drift
                if sweep == SWEEPS - 1:
                    stage[j, base + g] = latent(sweep, j, g)

        run_evals(evals, lhs, w_out_ref, done)
        for peer in others:
            @pl.when(peer != 0)
            def _(peer=peer):
                data_copy(group, me, peer).start()

        @pl.when(me != 0)
        def _():
            own_copy(group).start()

        return carry

    lax.fori_loop(0, n_groups, sweeps, 0)

    for peer in others:
        for copy in param_copies(me, peer):
            copy.wait_send()

    @pl.when(me == 0)
    def _():
        pltpu.make_async_copy(x_all, out_hbm, pass_sem).wait()

    def finish(group, carry):
        for peer in others:
            @pl.when(peer != 0)
            def _(peer=peer):
                data_copy(group, me, peer).wait_send()

        @pl.when(me != 0)
        def _():
            own_copy(group).wait()
            for peer in others:
                data_copy(group, peer, peer).wait_recv()

        return carry

    lax.fori_loop(0, n_groups, finish, 0)


def solution(mesh):
    def local(x_init, w_in, w_out, mod_scale, mod_shift, step_size):
        n_lat = x_init.shape[0]
        n_own = n_lat // N_TIME
        n_groups = n_own // GROUP
        out = pl.pallas_call(
            functools.partial(kernel, n_lat),
            out_shape=jax.ShapeDtypeStruct((n_lat, CH, TOK), jnp.float32),
            in_specs=[pl.BlockSpec(memory_space=pltpu.HBM)] * 6,
            out_specs=pl.BlockSpec(memory_space=pl.ANY),
            scratch_shapes=[
                pltpu.VMEM((CH, HIDDEN), jnp.bfloat16),
                pltpu.VMEM((CH, HIDDEN), jnp.bfloat16),
                pltpu.VMEM((n_own, CH, TOK), jnp.float32),
                pltpu.VMEM((n_lat, CH, TOK), jnp.float32),
                pltpu.VMEM((N_TIME, HIDDEN, DEPTH), jnp.bfloat16),
                pltpu.VMEM((N_TIME, n_own, CH, TOK), jnp.float32),
                pltpu.VMEM((N_TIME, n_own, CH, TOK), jnp.float32),
                pltpu.VMEM((N_TIME, 1, HIDDEN), jnp.bfloat16),
                pltpu.VMEM((N_TIME, 1, HIDDEN), jnp.bfloat16),
                pltpu.VMEM((N_TIME, 1, 1), jnp.float32),
                pltpu.SemaphoreType.DMA((6,)),
                pltpu.SemaphoreType.DMA,
                pltpu.SemaphoreType.DMA((n_groups,)),
                pltpu.SemaphoreType.DMA((3, N_TIME)),
                pltpu.SemaphoreType.DMA((3, N_TIME)),
                pltpu.SemaphoreType.DMA((n_groups, N_TIME)),
                pltpu.SemaphoreType.DMA((n_groups, N_TIME)),
            ],
            compiler_params=pltpu.CompilerParams(
                collective_id=0, has_side_effects=True,
                vmem_limit_bytes=67_043_328),
        )(jnp.transpose(x_init, (0, 2, 1)), w_in, w_out.T, mod_scale, mod_shift, step_size[:, None])
        return jnp.transpose(out, (0, 2, 1))[None]

    return jax.shard_map(local, mesh=mesh, in_specs=(P("data"), P(), P(), P("time"), P("time"), P("time")), out_specs=P("time", "data"), check_vma=False)
```

```python
import functools

import jax
import jax.numpy as jnp
from jax import lax
from jax.experimental import pallas as pl
from jax.experimental.pallas import tpu as pltpu
from jax.sharding import PartitionSpec as P

SWEEPS = 4
N_TIME = 4
CH = 16
TOK = 256
HIDDEN = 1152
BLOCK = 128
LAG = 5
GROUP = 5
LAST = 1
GROUP_A = 8
DEPTH = 8 * CH
SQRT_2_PI = 0.7978845608028654
LINEAR = 2.0 * SQRT_2_PI
CUBIC = 8.0 * 0.044715 * SQRT_2_PI
MESH = pl.DeviceIdType.MESH
UP = 2.0**64
DOWN = 2.0**-64
SPLIT = 0.5


def modulated_weights(w_in, scale, shift):
    half = 0.5 * (1.0 + scale.astype(jnp.float32))
    w = w_in.astype(jnp.float32)
    low = w * half
    high = (w * DOWN) * (half * DOWN)
    in_high = jnp.abs(high) >= SPLIT
    rows = []
    for chosen, value in ((jnp.logical_not(in_high), low), (in_high, high)):
        rest = jnp.where(chosen, value, 0.0)
        for _ in range(3):
            part = rest.astype(jnp.bfloat16)
            rest = rest - part.astype(jnp.float32)
            rows.append(part)
    first_row = lax.broadcasted_iota(jnp.int32, (CH, HIDDEN), 0) == 0
    half_shift = jnp.broadcast_to(0.5 * shift.astype(jnp.float32), (CH, HIDDEN))
    rows.append(jnp.where(first_row, half_shift, 0.0).astype(jnp.bfloat16))
    rows.append(jnp.zeros((CH, HIDDEN), jnp.bfloat16))
    return jnp.concatenate(rows, axis=0).T


def first_rhs(latent, ones):
    top = float(jnp.finfo(jnp.bfloat16).max)
    x = latent.astype(jnp.bfloat16)
    up = jnp.clip(x * UP * UP, -top, top)
    return jnp.concatenate([x, x, x, up, up, up, ones, jnp.zeros_like(ones)], axis=0)


def activation(half_pre):
    cubic = half_pre * (half_pre * half_pre * CUBIC + LINEAR)
    return (half_pre * jnp.tanh(cubic) + half_pre).astype(jnp.bfloat16)


def run_evals(evals, lhs, w_out_ref, done):
    n_blocks = HIDDEN // BLOCK
    steps = [(e, b) for e in range(len(evals)) for b in range(n_blocks)]
    pre, rhs, acc = {}, {}, {}

    def issue(limit):
        while len(pre) + done_steps[0] < min(limit, len(steps)):
            i = len(pre) + done_steps[0]
            e, b = steps[i]
            if b == 0:
                if not evals[e][3]():
                    return
                rhs[e] = evals[e][2]()
            pre[i] = jnp.dot(lhs(evals[e][1], b), rhs[e], preferred_element_type=jnp.float32)

    done_steps = [0]
    issue(LAG)
    for i, (e, b) in enumerate(steps):
        issue(i + LAG + 1)
        done_steps[0] = i + 1
        hidden = activation(pre.pop(i))
        part = jnp.dot(w_out_ref[:, b * BLOCK:(b + 1) * BLOCK], hidden, preferred_element_type=jnp.float32)
        acc[e] = part if b == 0 else acc[e] + part
        if b == n_blocks - 1:
            done(evals[e][0], acc.pop(e))


def kernel(n_lat, x_hbm, w_in_hbm, w_out_hbm, scale_hbm, shift_hbm, step_hbm, out_ref,
           w_in_ref, w_out_ref, x_own, lhs_ref, drift0, stage, scales, shifts, steps_buf,
           load_sem, pass_sem, par_send, par_recv, send_sem, recv_sem):
    me = lax.axis_index("time")
    others = [lax.rem(me + k, N_TIME) for k in range(1, N_TIME)]
    n_own = n_lat // N_TIME
    n_groups = n_own // GROUP
    assert n_groups * GROUP + LAST == n_own

    loads = [
        pltpu.make_async_copy(src, dst, load_sem.at[i])
        for i, (src, dst) in enumerate((
            (scale_hbm, scales.at[me]), (shift_hbm, shifts.at[me]), (step_hbm, steps_buf.at[me]),
            (w_in_hbm, w_in_ref), (x_hbm.at[pl.ds(me * n_own, n_own)], x_own), (w_out_hbm, w_out_ref)))
    ]
    for load in loads:
        load.start()
    barrier = pltpu.get_barrier_semaphore()
    for peer in others:
        pl.semaphore_signal(barrier, inc=1, device_id={"time": peer}, device_id_type=MESH)

    rest = pl.ds(n_own, n_lat - n_own)
    keep = pltpu.make_async_copy(x_hbm.at[rest], out_ref.at[rest], pass_sem)

    @pl.when(me == 0)
    def _():
        keep.start()

    for load in loads[:4]:
        load.wait()
    lhs_ref[me] = modulated_weights(w_in_ref[...], scales[me], shifts[me])
    pl.semaphore_wait(barrier, N_TIME - 1)

    def param_copies(slot, peer):
        return [
            pltpu.make_async_remote_copy(
                src_ref=dst.at[slot], dst_ref=dst.at[slot], send_sem=par_send.at[i, peer], recv_sem=par_recv.at[i, slot],
                device_id={"time": peer}, device_id_type=MESH)
            for i, dst in enumerate((scales, shifts, steps_buf))
        ]

    for peer in others:
        for copy in param_copies(me, peer):
            copy.start()
    for load in loads[4:]:
        load.wait()

    ones = (lax.broadcasted_iota(jnp.int32, (CH, TOK), 0) == 0).astype(jnp.float32).astype(jnp.bfloat16)

    def lhs(timestep, block):
        return lhs_ref[timestep, block * BLOCK:(block + 1) * BLOCK, :]

    def own_pass(trip, carry):
        base = trip * GROUP_A
        evals = [(base + g, me, functools.partial(lambda i: first_rhs(x_own[i], ones), base + g), lambda: True) for g in range(GROUP_A)]

        def done(i, drift):
            drift0[me, i] = drift

        run_evals(evals, lhs, w_out_ref, done)
        return carry

    lax.fori_loop(0, n_own // GROUP_A, own_pass, 0)

    for peer in others:
        for copy in param_copies(peer, peer):
            copy.wait_recv()
    for peer in others:
        lhs_ref[peer] = modulated_weights(w_in_ref[...], scales[peer], shifts[peer])
    half_step = [0.5 * steps_buf[j] for j in range(N_TIME - 1)]

    def data_copy(trip, size, slot, peer):
        base = trip * GROUP
        return pltpu.make_async_remote_copy(
            src_ref=stage.at[peer, pl.ds(base, size)], dst_ref=out_ref.at[pl.ds(slot * n_own + base, size)],
            send_sem=send_sem.at[trip, peer], recv_sem=recv_sem.at[trip, slot],
            device_id={"time": peer}, device_id_type=MESH)

    def sweeps(trip, size):
        base = trip * GROUP
        x0 = [x_own[base + g] for g in range(size)]
        drifts = {}
        evals = []
        rhs0 = {}

        def start_rhs(g):
            if g not in rhs0:
                rhs0[g] = first_rhs(x0[g], ones)
            return rhs0[g]

        def latent(sweep, j, g):
            total = x0[g]
            for i in range(j):
                total = total + half_step[i] * (drifts[sweep, i, g] + drifts[sweep, i + 1, g])
            return total

        for k in range(N_TIME - 1):
            for g in range(size):
                evals.append((("first", k, g), others[k], functools.partial(start_rhs, g), lambda: True))
        for sweep in range(1, SWEEPS):
            for g in range(size):
                for j in range(1, N_TIME):
                    evals.append(((sweep, j, g), j, functools.partial(
                        lambda s, j, g: first_rhs(latent(s - 1, j, g), ones), sweep, j, g), functools.partial(
                            lambda s, j, g: all((s - 1, i, g) in drifts for i in range(j + 1)), sweep, j, g)))

        def done(key, drift):
            if key[0] == "first":
                _, k, g = key
                drift0[others[k], base + g] = drift
                if k == N_TIME - 2:
                    for j in range(N_TIME):
                        drifts[0, j, g] = drift0[j, base + g]
                        if j == 0:
                            for sweep in range(1, SWEEPS):
                                drifts[sweep, 0, g] = drifts[0, 0, g]
            else:
                sweep, j, g = key
                drifts[sweep, j, g] = drift
                if sweep == SWEEPS - 1:
                    stage[j, base + g] = latent(sweep, j, g)
                    if j == 1:
                        stage[0, base + g] = x0[g]

        run_evals(evals, lhs, w_out_ref, done)
        for peer in others:
            @pl.when(peer != 0)
            def _(peer=peer):
                data_copy(trip, size, me, peer).start()

        for g in range(size):
            out_ref[me * n_own + base + g] = stage[me, base + g]

    def full_trip(trip, carry):
        sweeps(trip, GROUP)
        return carry

    lax.fori_loop(0, n_groups, full_trip, 0)
    sweeps(n_groups, LAST)

    for peer in others:
        for copy in param_copies(me, peer):
            copy.wait_send()

    @pl.when(me == 0)
    def _():
        keep.wait()

    def finish(trip, size):
        for peer in others:
            @pl.when(peer != 0)
            def _(peer=peer):
                data_copy(trip, size, me, peer).wait_send()

        @pl.when(me != 0)
        def _():
            for peer in others:
                data_copy(trip, size, peer, peer).wait_recv()

    def full_finish(trip, carry):
        finish(trip, GROUP)
        return carry

    lax.fori_loop(0, n_groups, full_finish, 0)
    finish(n_groups, LAST)


def solution(mesh):
    def local(x_init, w_in, w_out, mod_scale, mod_shift, step_size):
        n_lat = x_init.shape[0]
        n_own = n_lat // N_TIME
        n_groups = n_own // GROUP + 1
        out = pl.pallas_call(
            functools.partial(kernel, n_lat),
            out_shape=pltpu.VMEM((n_lat, CH, TOK), jnp.float32),
            in_specs=[pl.BlockSpec(memory_space=pltpu.HBM)] * 6,
            out_specs=pl.BlockSpec(memory_space=pltpu.VMEM),
            scratch_shapes=[
                pltpu.VMEM((CH, HIDDEN), jnp.bfloat16),
                pltpu.VMEM((CH, HIDDEN), jnp.bfloat16),
                pltpu.VMEM((n_own, CH, TOK), jnp.float32),
                pltpu.VMEM((N_TIME, HIDDEN, DEPTH), jnp.bfloat16),
                pltpu.VMEM((N_TIME, n_own, CH, TOK), jnp.float32),
                pltpu.VMEM((N_TIME, n_own, CH, TOK), jnp.float32),
                pltpu.VMEM((N_TIME, 1, HIDDEN), jnp.bfloat16),
                pltpu.VMEM((N_TIME, 1, HIDDEN), jnp.bfloat16),
                pltpu.VMEM((N_TIME, 1, 1), jnp.float32),
                pltpu.SemaphoreType.DMA((6,)),
                pltpu.SemaphoreType.DMA,
                pltpu.SemaphoreType.DMA((3, N_TIME)),
                pltpu.SemaphoreType.DMA((3, N_TIME)),
                pltpu.SemaphoreType.DMA((n_groups, N_TIME)),
                pltpu.SemaphoreType.DMA((n_groups, N_TIME)),
            ],
            compiler_params=pltpu.CompilerParams(
                collective_id=0, has_side_effects=True,
                vmem_limit_bytes=60_000_000),
        )(jnp.transpose(x_init, (0, 2, 1)), w_in, w_out.T, mod_scale, mod_shift, step_size[:, None])
        return jnp.transpose(out, (0, 2, 1))[None]

    return jax.shard_map(local, mesh=mesh, in_specs=(P("data"), P(), P(), P("time"), P("time"), P("time")), out_specs=P("time", "data"), check_vma=False)
```

```python
import functools

import jax
import jax.numpy as jnp
from jax import lax
from jax.experimental import pallas as pl
from jax.experimental.pallas import tpu as pltpu
from jax.sharding import PartitionSpec as P

SWEEPS = 4
N_TIME = 4
CH = 16
TOK = 256
HIDDEN = 1152
BLOCK = 128
LAG = 5
GROUP = 5
LAST = 1
DEPTH = 8 * CH
SQRT_2_PI = 0.7978845608028654
LINEAR = 2.0 * SQRT_2_PI
CUBIC = 8.0 * 0.044715 * SQRT_2_PI
MESH = pl.DeviceIdType.MESH
UP = 2.0**64
DOWN = 2.0**-64
SPLIT = 0.5


def modulated_weights(w_in, scale, shift):
    half = 0.5 * (1.0 + scale.astype(jnp.float32))
    w = w_in.astype(jnp.float32)
    low = w * half
    high = (w * DOWN) * (half * DOWN)
    in_high = jnp.abs(high) >= SPLIT
    rows = []
    for chosen, value in ((jnp.logical_not(in_high), low), (in_high, high)):
        rest = jnp.where(chosen, value, 0.0)
        for _ in range(3):
            part = rest.astype(jnp.bfloat16)
            rest = rest - part.astype(jnp.float32)
            rows.append(part)
    first_row = lax.broadcasted_iota(jnp.int32, (CH, HIDDEN), 0) == 0
    half_shift = jnp.broadcast_to(0.5 * shift.astype(jnp.float32), (CH, HIDDEN))
    rows.append(jnp.where(first_row, half_shift, 0.0).astype(jnp.bfloat16))
    rows.append(jnp.zeros((CH, HIDDEN), jnp.bfloat16))
    return jnp.concatenate(rows, axis=0).T


def first_rhs(latent, ones):
    top = float(jnp.finfo(jnp.bfloat16).max)
    x = latent.astype(jnp.bfloat16)
    up = jnp.clip(x * UP * UP, -top, top)
    return jnp.concatenate([x, x, x, up, up, up, ones, jnp.zeros_like(ones)], axis=0)


def activation(half_pre):
    cubic = half_pre * (half_pre * half_pre * CUBIC + LINEAR)
    return (half_pre * jnp.tanh(cubic) + half_pre).astype(jnp.bfloat16)


def run_evals(evals, lhs, w_out_ref, done):
    n_blocks = HIDDEN // BLOCK
    steps = [(e, b) for e in range(len(evals)) for b in range(n_blocks)]
    pre, rhs, acc = {}, {}, {}

    def issue(limit):
        while len(pre) + done_steps[0] < min(limit, len(steps)):
            i = len(pre) + done_steps[0]
            e, b = steps[i]
            if b == 0:
                if not evals[e][3]():
                    return
                rhs[e] = evals[e][2]()
            pre[i] = jnp.dot(lhs(evals[e][1], b), rhs[e], preferred_element_type=jnp.float32)

    done_steps = [0]
    issue(LAG)
    for i, (e, b) in enumerate(steps):
        issue(i + LAG + 1)
        done_steps[0] = i + 1
        hidden = activation(pre.pop(i))
        part = jnp.dot(w_out_ref[:, b * BLOCK:(b + 1) * BLOCK], hidden, preferred_element_type=jnp.float32)
        acc[e] = part if b == 0 else acc[e] + part
        if b == n_blocks - 1:
            done(evals[e][0], acc.pop(e))


def kernel(n_lat, x_hbm, w_in_hbm, w_out_hbm, scale_hbm, shift_hbm, step_hbm, out_ref,
           w_in_ref, w_out_ref, x_own, lhs_ref, drift0, stage, scale_ref, shift_ref, step_ref, params,
           load_sem, pass_sem, par_send, par_recv, send_sem, recv_sem):
    me = lax.axis_index("time")
    others = [lax.rem(me + k, N_TIME) for k in range(1, N_TIME)]
    n_own = n_lat // N_TIME
    n_groups = n_own // GROUP
    assert n_groups * GROUP + LAST == n_own

    loads = [
        pltpu.make_async_copy(src, dst, load_sem.at[i])
        for i, (src, dst) in enumerate((
            (scale_hbm, scale_ref), (shift_hbm, shift_ref), (step_hbm, step_ref),
            (w_in_hbm, w_in_ref), (x_hbm.at[pl.ds(me * n_own, n_own)], x_own), (w_out_hbm, w_out_ref)))
    ]
    for load in loads:
        load.start()
    barrier = pltpu.get_barrier_semaphore()
    for peer in others:
        pl.semaphore_signal(barrier, inc=1, device_id={"time": peer}, device_id_type=MESH)

    rest = pl.ds(n_own, n_lat - n_own)
    keep = pltpu.make_async_copy(x_hbm.at[rest], out_ref.at[rest], pass_sem)

    @pl.when(me == 0)
    def _():
        keep.start()

    for load in loads[:4]:
        load.wait()
    row = (1, HIDDEN)
    params[me] = jnp.concatenate([
        scale_ref[...].astype(jnp.float32), shift_ref[...].astype(jnp.float32),
        jnp.broadcast_to(step_ref[...], row), jnp.zeros(row, jnp.float32)], axis=0)
    lhs_ref[me] = modulated_weights(w_in_ref[...], scale_ref[...], shift_ref[...])
    def param_copy(slot, peer):
        return pltpu.make_async_remote_copy(
            src_ref=params.at[slot], dst_ref=params.at[slot], send_sem=par_send.at[peer], recv_sem=par_recv.at[slot],
            device_id={"time": peer}, device_id_type=MESH)

    for load in loads[4:]:
        load.wait()

    ones = (lax.broadcasted_iota(jnp.int32, (CH, TOK), 0) == 0).astype(jnp.float32).astype(jnp.bfloat16)

    def lhs(timestep, block):
        return lhs_ref[timestep, block * BLOCK:(block + 1) * BLOCK, :]

    def own_pass(latents):
        def done(i, drift):
            drift0[me, i] = drift

        evals = [(i, me, functools.partial(lambda i: first_rhs(x_own[i], ones), i), lambda: True) for i in latents]
        run_evals(evals, lhs, w_out_ref, done)

    pl.semaphore_wait(barrier, N_TIME - 1)
    for peer in others:
        param_copy(me, peer).start()
    own_pass(range(n_own))

    for peer in others:
        param_copy(peer, peer).wait_recv()
    for peer in others:
        lhs_ref[peer] = modulated_weights(w_in_ref[...], params[peer, 0:1], params[peer, 1:2])
    half_step = [0.5 * params[j, 2:3, 0:1] for j in range(N_TIME - 1)]

    def data_copy(trip, size, slot, peer):
        base = trip * GROUP
        return pltpu.make_async_remote_copy(
            src_ref=stage.at[peer, pl.ds(base, size)], dst_ref=out_ref.at[pl.ds(slot * n_own + base, size)],
            send_sem=send_sem.at[trip, peer], recv_sem=recv_sem.at[trip, slot],
            device_id={"time": peer}, device_id_type=MESH)

    def sweeps(trip, size):
        base = trip * GROUP
        x0 = [x_own[base + g] for g in range(size)]
        drifts = {}
        evals = []
        rhs0 = {}

        def start_rhs(g):
            if g not in rhs0:
                rhs0[g] = first_rhs(x0[g], ones)
            return rhs0[g]

        def latent(sweep, j, g):
            total = x0[g]
            for i in range(j):
                total = total + half_step[i] * (drifts[sweep, i, g] + drifts[sweep, i + 1, g])
            return total

        for k in range(N_TIME - 1):
            for g in range(size):
                evals.append((("first", k, g), others[k], functools.partial(start_rhs, g), lambda: True))
        for sweep in range(1, SWEEPS):
            for g in range(size):
                for j in range(1, N_TIME):
                    evals.append(((sweep, j, g), j, functools.partial(
                        lambda s, j, g: first_rhs(latent(s - 1, j, g), ones), sweep, j, g), functools.partial(
                            lambda s, j, g: all((s - 1, i, g) in drifts for i in range(j + 1)), sweep, j, g)))

        def done(key, drift):
            if key[0] == "first":
                _, k, g = key
                drift0[others[k], base + g] = drift
                if k == N_TIME - 2:
                    for j in range(N_TIME):
                        drifts[0, j, g] = drift0[j, base + g]
                        if j == 0:
                            for sweep in range(1, SWEEPS):
                                drifts[sweep, 0, g] = drifts[0, 0, g]
            else:
                sweep, j, g = key
                drifts[sweep, j, g] = drift
                if sweep == SWEEPS - 1:
                    stage[j, base + g] = latent(sweep, j, g)
                    if j == 1:
                        stage[0, base + g] = x0[g]

        run_evals(evals, lhs, w_out_ref, done)
        for peer in others:
            @pl.when(peer != 0)
            def _(peer=peer):
                data_copy(trip, size, me, peer).start()

        for g in range(size):
            out_ref[me * n_own + base + g] = stage[me, base + g]

    def full_trip(trip, carry):
        sweeps(trip, GROUP)
        return carry

    lax.fori_loop(0, n_groups, full_trip, 0)
    sweeps(n_groups, LAST)

    for peer in others:
        param_copy(me, peer).wait_send()

    @pl.when(me == 0)
    def _():
        keep.wait()

    def finish(trip, size):
        for peer in others:
            @pl.when(peer != 0)
            def _(peer=peer):
                data_copy(trip, size, me, peer).wait_send()

        @pl.when(me != 0)
        def _():
            for peer in others:
                data_copy(trip, size, peer, peer).wait_recv()

    def full_finish(trip, carry):
        finish(trip, GROUP)
        return carry

    lax.fori_loop(0, n_groups, full_finish, 0)
    finish(n_groups, LAST)


def solution(mesh):
    def local(x_init, w_in, w_out, mod_scale, mod_shift, step_size):
        n_lat = x_init.shape[0]
        n_own = n_lat // N_TIME
        n_groups = n_own // GROUP + 1
        out = pl.pallas_call(
            functools.partial(kernel, n_lat),
            out_shape=pltpu.VMEM((n_lat, CH, TOK), jnp.float32),
            in_specs=[pl.BlockSpec(memory_space=pltpu.HBM)] * 6,
            out_specs=pl.BlockSpec(memory_space=pltpu.VMEM),
            scratch_shapes=[
                pltpu.VMEM((CH, HIDDEN), jnp.bfloat16),
                pltpu.VMEM((CH, HIDDEN), jnp.bfloat16),
                pltpu.VMEM((n_own, CH, TOK), jnp.float32),
                pltpu.VMEM((N_TIME, HIDDEN, DEPTH), jnp.bfloat16),
                pltpu.VMEM((N_TIME, n_own, CH, TOK), jnp.float32),
                pltpu.VMEM((N_TIME, n_own, CH, TOK), jnp.float32),
                pltpu.VMEM((1, HIDDEN), jnp.bfloat16),
                pltpu.VMEM((1, HIDDEN), jnp.bfloat16),
                pltpu.VMEM((1, 1), jnp.float32),
                pltpu.VMEM((N_TIME, 4, HIDDEN), jnp.float32),
                pltpu.SemaphoreType.DMA((6,)),
                pltpu.SemaphoreType.DMA,
                pltpu.SemaphoreType.DMA((N_TIME,)),
                pltpu.SemaphoreType.DMA((N_TIME,)),
                pltpu.SemaphoreType.DMA((n_groups, N_TIME)),
                pltpu.SemaphoreType.DMA((n_groups, N_TIME)),
            ],
            compiler_params=pltpu.CompilerParams(
                collective_id=0, has_side_effects=True,
                vmem_limit_bytes=60_000_000),
        )(jnp.transpose(x_init, (0, 2, 1)), w_in, w_out.T, mod_scale, mod_shift, step_size[:, None])
        return jnp.transpose(out, (0, 2, 1))[None]

    return jax.shard_map(local, mesh=mesh, in_specs=(P("data"), P(), P(), P("time"), P("time"), P("time")), out_specs=P("time", "data"), check_vma=False)
```

```python
import functools

import jax
import jax.numpy as jnp
from jax import lax
from jax.experimental import pallas as pl
from jax.experimental.pallas import tpu as pltpu
from jax.sharding import PartitionSpec as P

SWEEPS = 4
N_TIME = 4
CH = 16
TOK = 256
HIDDEN = 1152
BLOCK = 128
LAG = 5
GROUP = 5
LAST = 1
DEPTH = 8 * CH
SQRT_2_PI = 0.7978845608028654
LINEAR = 2.0 * SQRT_2_PI
CUBIC = 8.0 * 0.044715 * SQRT_2_PI
MESH = pl.DeviceIdType.MESH
UP = 2.0**64
DOWN = 2.0**-64
SPLIT = 0.5


def modulated_weights(w_in, scale, shift):
    half = 0.5 * (1.0 + scale.astype(jnp.float32))
    w = w_in.astype(jnp.float32)
    low = w * half
    high = (w * DOWN) * (half * DOWN)
    in_high = jnp.abs(high) >= SPLIT
    rows = []
    for chosen, value in ((jnp.logical_not(in_high), low), (in_high, high)):
        rest = jnp.where(chosen, value, 0.0)
        for _ in range(3):
            part = rest.astype(jnp.bfloat16)
            rest = rest - part.astype(jnp.float32)
            rows.append(part)
    first_row = lax.broadcasted_iota(jnp.int32, (CH, HIDDEN), 0) == 0
    half_shift = jnp.broadcast_to(0.5 * shift.astype(jnp.float32), (CH, HIDDEN))
    rows.append(jnp.where(first_row, half_shift, 0.0).astype(jnp.bfloat16))
    rows.append(jnp.zeros((CH, HIDDEN), jnp.bfloat16))
    return jnp.concatenate(rows, axis=0).T


def first_rhs(latent, ones):
    top = float(jnp.finfo(jnp.bfloat16).max)
    x = latent.astype(jnp.bfloat16)
    up = jnp.clip(x * UP * UP, -top, top)
    return jnp.concatenate([x, x, x, up, up, up, ones, jnp.zeros_like(ones)], axis=0)


def activation(half_pre):
    cubic = half_pre * (half_pre * half_pre * CUBIC + LINEAR)
    return (half_pre * jnp.tanh(cubic) + half_pre).astype(jnp.bfloat16)


def run_evals(evals, lhs, w_out_ref, done):
    n_blocks = HIDDEN // BLOCK
    steps = [(e, b) for e in range(len(evals)) for b in range(n_blocks)]
    pre, rhs, acc = {}, {}, {}

    def issue(limit):
        while len(pre) + done_steps[0] < min(limit, len(steps)):
            i = len(pre) + done_steps[0]
            e, b = steps[i]
            if b == 0:
                if not evals[e][3]():
                    return
                rhs[e] = evals[e][2]()
            pre[i] = jnp.dot(lhs(evals[e][1], b), rhs[e], preferred_element_type=jnp.float32)

    done_steps = [0]
    issue(LAG)
    for i, (e, b) in enumerate(steps):
        issue(i + LAG + 1)
        done_steps[0] = i + 1
        hidden = activation(pre.pop(i))
        part = jnp.dot(w_out_ref[:, b * BLOCK:(b + 1) * BLOCK], hidden, preferred_element_type=jnp.float32)
        acc[e] = part if b == 0 else acc[e] + part
        if b == n_blocks - 1:
            done(evals[e][0], acc.pop(e))


def kernel(n_lat, x_hbm, w_in_hbm, w_out_hbm, scale_hbm, shift_hbm, step_hbm, out_ref,
           w_in_ref, w_out_ref, x_own, lhs_ref, drift0, stage, scale_ref, shift_ref, step_ref, params,
           load_sem, pass_sem, par_send, par_recv, send_sem, recv_sem):
    me = lax.axis_index("time")
    others = [lax.rem(me + k, N_TIME) for k in range(1, N_TIME)]
    n_own = n_lat // N_TIME
    n_groups = n_own // GROUP
    assert n_groups * GROUP + LAST == n_own

    loads = [
        pltpu.make_async_copy(src, dst, load_sem.at[i])
        for i, (src, dst) in enumerate((
            (scale_hbm, scale_ref), (shift_hbm, shift_ref), (step_hbm, step_ref),
            (w_in_hbm, w_in_ref), (x_hbm.at[pl.ds(me * n_own, n_own)], x_own), (w_out_hbm, w_out_ref)))
    ]
    for load in loads:
        load.start()
    barrier = pltpu.get_barrier_semaphore()
    for peer in others:
        pl.semaphore_signal(barrier, inc=1, device_id={"time": peer}, device_id_type=MESH)

    rest = pl.ds(n_own, n_lat - n_own)
    keep = pltpu.make_async_copy(x_hbm.at[rest], out_ref.at[rest], pass_sem)

    @pl.when(me == 0)
    def _():
        keep.start()

    for load in loads[:4]:
        load.wait()
    row = (1, HIDDEN)
    params[me] = jnp.concatenate([
        scale_ref[...].astype(jnp.float32), shift_ref[...].astype(jnp.float32),
        jnp.broadcast_to(step_ref[...], row), jnp.zeros(row, jnp.float32)], axis=0)
    lhs_ref[me] = modulated_weights(w_in_ref[...], scale_ref[...], shift_ref[...])
    def param_copy(slot, peer):
        return pltpu.make_async_remote_copy(
            src_ref=params.at[slot], dst_ref=params.at[slot], send_sem=par_send.at[peer], recv_sem=par_recv.at[slot],
            device_id={"time": peer}, device_id_type=MESH)

    for load in loads[4:]:
        load.wait()

    ones = (lax.broadcasted_iota(jnp.int32, (CH, TOK), 0) == 0).astype(jnp.float32).astype(jnp.bfloat16)

    def lhs(timestep, block):
        return lhs_ref[timestep, block * BLOCK:(block + 1) * BLOCK, :]

    def own_pass(latents):
        def done(i, drift):
            drift0[me, i] = drift

        evals = [(i, me, functools.partial(lambda i: first_rhs(x_own[i], ones), i), lambda: True) for i in latents]
        run_evals(evals, lhs, w_out_ref, done)

    pl.semaphore_wait(barrier, N_TIME - 1)
    for peer in others:
        param_copy(me, peer).start()
    own_pass(range(n_own))

    for peer in others:
        param_copy(peer, peer).wait_recv()
    for peer in others:
        lhs_ref[peer] = modulated_weights(w_in_ref[...], params[peer, 0:1], params[peer, 1:2])
    half_step = [0.5 * params[j, 2:3, 0:1] for j in range(N_TIME - 1)]

    def data_copy(trip, size, slot, peer):
        base = trip * GROUP
        return pltpu.make_async_remote_copy(
            src_ref=stage.at[peer, pl.ds(base, size)], dst_ref=out_ref.at[pl.ds(slot * n_own + base, size)],
            send_sem=send_sem.at[trip, peer], recv_sem=recv_sem.at[trip, slot],
            device_id={"time": peer}, device_id_type=MESH)

    def sweeps(trip, size):
        base = trip * GROUP
        x0 = [x_own[base + g] for g in range(size)]
        drifts = {}
        evals = []
        rhs0 = {}

        def start_rhs(g):
            if g not in rhs0:
                rhs0[g] = first_rhs(x0[g], ones)
            return rhs0[g]

        def latent(sweep, j, g):
            total = x0[g]
            for i in range(j):
                total = total + half_step[i] * (drifts[sweep, i, g] + drifts[sweep, i + 1, g])
            return total

        for k in range(N_TIME - 1):
            for g in range(size):
                evals.append((("first", k, g), others[k], functools.partial(start_rhs, g), lambda: True))
        for sweep in range(1, SWEEPS):
            for g in range(size):
                for j in range(1, N_TIME):
                    evals.append(((sweep, j, g), j, functools.partial(
                        lambda s, j, g: first_rhs(latent(s - 1, j, g), ones), sweep, j, g), functools.partial(
                            lambda s, j, g: all((s - 1, i, g) in drifts for i in range(j + 1)), sweep, j, g)))

        def done(key, drift):
            if key[0] == "first":
                _, k, g = key
                drift0[others[k], base + g] = drift
                if k == N_TIME - 2:
                    for j in range(N_TIME):
                        drifts[0, j, g] = drift0[j, base + g]
                        if j == 0:
                            for sweep in range(1, SWEEPS):
                                drifts[sweep, 0, g] = drifts[0, 0, g]
            else:
                sweep, j, g = key
                drifts[sweep, j, g] = drift
                if sweep == SWEEPS - 1:
                    stage[j, base + g] = latent(sweep, j, g)
                    if j == 1:
                        stage[0, base + g] = x0[g]
                    if size == LAST:
                        @pl.when(me != j)
                        def _():
                            data_copy(trip, size, me, j).start()

        run_evals(evals, lhs, w_out_ref, done)
        for peer in others if size != LAST else ():
            @pl.when(peer != 0)
            def _(peer=peer):
                data_copy(trip, size, me, peer).start()

        for g in range(size):
            out_ref[me * n_own + base + g] = stage[me, base + g]

    def full_trip(trip, carry):
        sweeps(trip, GROUP)
        return carry

    lax.fori_loop(0, n_groups, full_trip, 0)
    sweeps(n_groups, LAST)

    for peer in others:
        param_copy(me, peer).wait_send()

    @pl.when(me == 0)
    def _():
        keep.wait()

    def finish(trip, size):
        for peer in others:
            @pl.when(peer != 0)
            def _(peer=peer):
                data_copy(trip, size, me, peer).wait_send()

        @pl.when(me != 0)
        def _():
            for peer in others:
                data_copy(trip, size, peer, peer).wait_recv()

    def full_finish(trip, carry):
        finish(trip, GROUP)
        return carry

    lax.fori_loop(0, n_groups, full_finish, 0)
    finish(n_groups, LAST)


def solution(mesh):
    def local(x_init, w_in, w_out, mod_scale, mod_shift, step_size):
        n_lat = x_init.shape[0]
        n_own = n_lat // N_TIME
        n_groups = n_own // GROUP + 1
        out = pl.pallas_call(
            functools.partial(kernel, n_lat),
            out_shape=pltpu.VMEM((n_lat, CH, TOK), jnp.float32),
            in_specs=[pl.BlockSpec(memory_space=pltpu.HBM)] * 6,
            out_specs=pl.BlockSpec(memory_space=pltpu.VMEM),
            scratch_shapes=[
                pltpu.VMEM((CH, HIDDEN), jnp.bfloat16),
                pltpu.VMEM((CH, HIDDEN), jnp.bfloat16),
                pltpu.VMEM((n_own, CH, TOK), jnp.float32),
                pltpu.VMEM((N_TIME, HIDDEN, DEPTH), jnp.bfloat16),
                pltpu.VMEM((N_TIME, n_own, CH, TOK), jnp.float32),
                pltpu.VMEM((N_TIME, n_own, CH, TOK), jnp.float32),
                pltpu.VMEM((1, HIDDEN), jnp.bfloat16),
                pltpu.VMEM((1, HIDDEN), jnp.bfloat16),
                pltpu.VMEM((1, 1), jnp.float32),
                pltpu.VMEM((N_TIME, 4, HIDDEN), jnp.float32),
                pltpu.SemaphoreType.DMA((6,)),
                pltpu.SemaphoreType.DMA,
                pltpu.SemaphoreType.DMA((N_TIME,)),
                pltpu.SemaphoreType.DMA((N_TIME,)),
                pltpu.SemaphoreType.DMA((n_groups, N_TIME)),
                pltpu.SemaphoreType.DMA((n_groups, N_TIME)),
            ],
            compiler_params=pltpu.CompilerParams(
                collective_id=0, has_side_effects=True,
                vmem_limit_bytes=60_000_000),
        )(jnp.transpose(x_init, (0, 2, 1)), w_in, w_out.T, mod_scale, mod_shift, step_size[:, None])
        return jnp.transpose(out, (0, 2, 1))[None]

    return jax.shard_map(local, mesh=mesh, in_specs=(P("data"), P(), P(), P("time"), P("time"), P("time")), out_specs=P("time", "data"), check_vma=False)
```

```python
import functools

import jax
import jax.numpy as jnp
from jax import lax
from jax.experimental import pallas as pl
from jax.experimental.pallas import tpu as pltpu
from jax.sharding import PartitionSpec as P

SWEEPS = 4
N_TIME = 4
CH = 16
TOK = 256
HIDDEN = 1152
BLOCK = 128
LAG = 5
GROUP = 5
LAST = 1
DEPTH = 8 * CH
SQRT_2_PI = 0.7978845608028654
LINEAR = 2.0 * SQRT_2_PI
CUBIC = 8.0 * 0.044715 * SQRT_2_PI
MESH = pl.DeviceIdType.MESH
UP = 2.0**64
DOWN = 2.0**-64
SPLIT = 0.5


def modulated_weights(w_in, scale, shift):
    half = 0.5 * (1.0 + scale.astype(jnp.float32))
    w = w_in.astype(jnp.float32)
    low = w * half
    high = (w * DOWN) * (half * DOWN)
    in_high = jnp.abs(high) >= SPLIT
    rows = []
    for chosen, value in ((jnp.logical_not(in_high), low), (in_high, high)):
        rest = jnp.where(chosen, value, 0.0)
        for _ in range(3):
            part = rest.astype(jnp.bfloat16)
            rest = rest - part.astype(jnp.float32)
            rows.append(part)
    first_row = lax.broadcasted_iota(jnp.int32, (CH, HIDDEN), 0) == 0
    half_shift = jnp.broadcast_to(0.5 * shift.astype(jnp.float32), (CH, HIDDEN))
    rows.append(jnp.where(first_row, half_shift, 0.0).astype(jnp.bfloat16))
    rows.append(jnp.zeros((CH, HIDDEN), jnp.bfloat16))
    return jnp.concatenate(rows, axis=0).T


def first_rhs(latent, ones):
    top = float(jnp.finfo(jnp.bfloat16).max)
    x = latent.astype(jnp.bfloat16)
    up = jnp.clip(x * UP * UP, -top, top)
    return jnp.concatenate([x, x, x, up, up, up, ones, jnp.zeros_like(ones)], axis=0)


def activation(half_pre):
    cubic = half_pre * (half_pre * half_pre * CUBIC + LINEAR)
    return (half_pre * jnp.tanh(cubic) + half_pre).astype(jnp.bfloat16)


def run_evals(evals, lhs, w_out_ref, done):
    n_blocks = HIDDEN // BLOCK
    steps = [(e, b) for e in range(len(evals)) for b in range(n_blocks)]
    pre, rhs, acc = {}, {}, {}

    def issue(limit):
        while len(pre) + done_steps[0] < min(limit, len(steps)):
            i = len(pre) + done_steps[0]
            e, b = steps[i]
            if b == 0:
                if not evals[e][3]():
                    return
                rhs[e] = evals[e][2]()
            pre[i] = jnp.dot(lhs(evals[e][1], b), rhs[e], preferred_element_type=jnp.float32)

    done_steps = [0]
    issue(LAG)
    for i, (e, b) in enumerate(steps):
        issue(i + LAG + 1)
        done_steps[0] = i + 1
        hidden = activation(pre.pop(i))
        part = jnp.dot(w_out_ref[:, b * BLOCK:(b + 1) * BLOCK], hidden, preferred_element_type=jnp.float32)
        acc[e] = part if b == 0 else acc[e] + part
        if b == n_blocks - 1:
            done(evals[e][0], acc.pop(e))


def kernel(n_lat, x_hbm, w_in_hbm, w_out_hbm, scale_hbm, shift_hbm, step_hbm, out_ref,
           w_in_ref, w_out_ref, x_own, lhs_ref, drift0, stage, scale_ref, shift_ref, step_ref, params,
           load_sem, pass_sem, par_send, par_recv, send_sem, recv_sem):
    me = lax.axis_index("time")
    others = [lax.rem(me + k, N_TIME) for k in range(1, N_TIME)]
    n_own = n_lat // N_TIME
    n_groups = n_own // GROUP
    assert n_groups * GROUP + LAST == n_own

    loads = [
        pltpu.make_async_copy(src, dst, load_sem.at[i])
        for i, (src, dst) in enumerate((
            (scale_hbm, scale_ref), (shift_hbm, shift_ref), (step_hbm, step_ref),
            (w_in_hbm, w_in_ref), (x_hbm.at[pl.ds(me * n_own, n_own)], x_own), (w_out_hbm, w_out_ref)))
    ]
    for load in loads:
        load.start()
    barrier = pltpu.get_barrier_semaphore()
    for peer in others:
        pl.semaphore_signal(barrier, inc=1, device_id={"time": peer}, device_id_type=MESH)

    rest = pl.ds(n_own, n_lat - n_own)
    keep = pltpu.make_async_copy(x_hbm.at[rest], out_ref.at[rest], pass_sem)

    @pl.when(me == 0)
    def _():
        keep.start()

    for load in loads[:4]:
        load.wait()
    row = (1, HIDDEN)
    params[me] = jnp.concatenate([
        scale_ref[...].astype(jnp.float32), shift_ref[...].astype(jnp.float32),
        jnp.broadcast_to(step_ref[...], row), jnp.zeros(row, jnp.float32)], axis=0)
    lhs_ref[me] = modulated_weights(w_in_ref[...], scale_ref[...], shift_ref[...])
    def param_copy(slot, peer):
        return pltpu.make_async_remote_copy(
            src_ref=params.at[slot], dst_ref=params.at[slot], send_sem=par_send.at[peer], recv_sem=par_recv.at[slot],
            device_id={"time": peer}, device_id_type=MESH)

    for load in loads[4:]:
        load.wait()

    ones = (lax.broadcasted_iota(jnp.int32, (CH, TOK), 0) == 0).astype(jnp.float32).astype(jnp.bfloat16)

    def lhs(timestep, block):
        return lhs_ref[timestep, block * BLOCK:(block + 1) * BLOCK, :]

    def own_pass(latents):
        def done(i, drift):
            drift0[me, i] = drift

        evals = [(i, me, functools.partial(lambda i: first_rhs(x_own[i], ones), i), lambda: True) for i in latents]
        run_evals(evals, lhs, w_out_ref, done)

    pl.semaphore_wait(barrier, N_TIME - 1)
    for peer in others:
        param_copy(me, peer).start()
    own_pass(range(n_own - 4))

    for peer in others:
        param_copy(peer, peer).wait_recv()
    own_pass(range(n_own - 4, n_own))
    for peer in others:
        lhs_ref[peer] = modulated_weights(w_in_ref[...], params[peer, 0:1], params[peer, 1:2])
    half_step = [0.5 * params[j, 2:3, 0:1] for j in range(N_TIME - 1)]

    def data_copy(trip, size, slot, peer):
        base = trip * GROUP
        return pltpu.make_async_remote_copy(
            src_ref=stage.at[peer, pl.ds(base, size)], dst_ref=out_ref.at[pl.ds(slot * n_own + base, size)],
            send_sem=send_sem.at[trip, peer], recv_sem=recv_sem.at[trip, slot],
            device_id={"time": peer}, device_id_type=MESH)

    def sweeps(trip, size):
        base = trip * GROUP
        x0 = [x_own[base + g] for g in range(size)]
        drifts = {}
        evals = []
        rhs0 = {}

        def start_rhs(g):
            if g not in rhs0:
                rhs0[g] = first_rhs(x0[g], ones)
            return rhs0[g]

        def latent(sweep, j, g):
            total = x0[g]
            for i in range(j):
                total = total + half_step[i] * (drifts[sweep, i, g] + drifts[sweep, i + 1, g])
            return total

        for k in range(N_TIME - 1):
            for g in range(size):
                evals.append((("first", k, g), others[k], functools.partial(start_rhs, g), lambda: True))
        for sweep in range(1, SWEEPS):
            for g in range(size):
                for j in range(1, N_TIME):
                    evals.append(((sweep, j, g), j, functools.partial(
                        lambda s, j, g: first_rhs(latent(s - 1, j, g), ones), sweep, j, g), functools.partial(
                            lambda s, j, g: all((s - 1, i, g) in drifts for i in range(j + 1)), sweep, j, g)))

        def done(key, drift):
            if key[0] == "first":
                _, k, g = key
                drift0[others[k], base + g] = drift
                if k == N_TIME - 2:
                    for j in range(N_TIME):
                        drifts[0, j, g] = drift0[j, base + g]
                        if j == 0:
                            for sweep in range(1, SWEEPS):
                                drifts[sweep, 0, g] = drifts[0, 0, g]
            else:
                sweep, j, g = key
                drifts[sweep, j, g] = drift
                if sweep == SWEEPS - 1:
                    stage[j, base + g] = latent(sweep, j, g)
                    if j == 1:
                        stage[0, base + g] = x0[g]
                    if size == LAST:
                        @pl.when(me != j)
                        def _():
                            data_copy(trip, size, me, j).start()

        run_evals(evals, lhs, w_out_ref, done)
        for peer in others if size != LAST else ():
            @pl.when(peer != 0)
            def _(peer=peer):
                data_copy(trip, size, me, peer).start()

        for g in range(size):
            out_ref[me * n_own + base + g] = stage[me, base + g]

    def full_trip(trip, carry):
        sweeps(trip, GROUP)
        return carry

    lax.fori_loop(0, n_groups, full_trip, 0)
    sweeps(n_groups, LAST)

    for peer in others:
        param_copy(me, peer).wait_send()

    @pl.when(me == 0)
    def _():
        keep.wait()

    def finish(trip, size):
        for peer in others:
            @pl.when(peer != 0)
            def _(peer=peer):
                data_copy(trip, size, me, peer).wait_send()

        @pl.when(me != 0)
        def _():
            for peer in others:
                data_copy(trip, size, peer, peer).wait_recv()

    def full_finish(trip, carry):
        finish(trip, GROUP)
        return carry

    lax.fori_loop(0, n_groups, full_finish, 0)
    finish(n_groups, LAST)


def solution(mesh):
    def local(x_init, w_in, w_out, mod_scale, mod_shift, step_size):
        n_lat = x_init.shape[0]
        n_own = n_lat // N_TIME
        n_groups = n_own // GROUP + 1
        out = pl.pallas_call(
            functools.partial(kernel, n_lat),
            out_shape=pltpu.VMEM((n_lat, CH, TOK), jnp.float32),
            in_specs=[pl.BlockSpec(memory_space=pltpu.HBM)] * 6,
            out_specs=pl.BlockSpec(memory_space=pltpu.VMEM),
            scratch_shapes=[
                pltpu.VMEM((CH, HIDDEN), jnp.bfloat16),
                pltpu.VMEM((CH, HIDDEN), jnp.bfloat16),
                pltpu.VMEM((n_own, CH, TOK), jnp.float32),
                pltpu.VMEM((N_TIME, HIDDEN, DEPTH), jnp.bfloat16),
                pltpu.VMEM((N_TIME, n_own, CH, TOK), jnp.float32),
                pltpu.VMEM((N_TIME, n_own, CH, TOK), jnp.float32),
                pltpu.VMEM((1, HIDDEN), jnp.bfloat16),
                pltpu.VMEM((1, HIDDEN), jnp.bfloat16),
                pltpu.VMEM((1, 1), jnp.float32),
                pltpu.VMEM((N_TIME, 4, HIDDEN), jnp.float32),
                pltpu.SemaphoreType.DMA((6,)),
                pltpu.SemaphoreType.DMA,
                pltpu.SemaphoreType.DMA((N_TIME,)),
                pltpu.SemaphoreType.DMA((N_TIME,)),
                pltpu.SemaphoreType.DMA((n_groups, N_TIME)),
                pltpu.SemaphoreType.DMA((n_groups, N_TIME)),
            ],
            compiler_params=pltpu.CompilerParams(
                collective_id=0, has_side_effects=True,
                vmem_limit_bytes=60_000_000),
        )(jnp.transpose(x_init, (0, 2, 1)), w_in, w_out.T, mod_scale, mod_shift, step_size[:, None])
        return jnp.transpose(out, (0, 2, 1))[None]

    return jax.shard_map(local, mesh=mesh, in_specs=(P("data"), P(), P(), P("time"), P("time"), P("time")), out_specs=P("time", "data"), check_vma=False)
```
